256 devices in a mesh: dp: 2 (over x_lo), expert: 128 (over y, z, x_hi, core).
Axes of the slice: x: 4 (x_hi: 2, x_lo: 2; x = x_hi * 2 + x_lo), y: 4, z: 8, core: 2. Of those that a mesh axis runs over, the one named last changes fastest.
Arguments:
- tokens: bfloat16 [256, 256, 1280], P(('dp', 'expert')), may hold values from -12 to 12
- router: bfloat16 [1280, 128], replicated, may hold values from -3 to 3
- w_in: bfloat16 [128, 1280, 5120], P('expert', None, 'dp'), may hold values from -0.15625 to 0.15625
- b_in: bfloat16 [128, 5120], P('expert'), may hold values from -3 to 3
- w_out: bfloat16 [128, 5120, 1280], P('expert', 'dp'), may hold values from -0.078125 to 0.078125
- b_out: bfloat16 [128, 1280], P('expert'), may hold values from -3 to 3
Outputs:
- mixed: bfloat16 [256, 256, 1280], P(('dp', 'expert'))
The draws below stay inside these ranges and needn't reach their ends.
All inputs are finite; a program needn't handle non-finite values.
Results may differ from the reference program's by a relative error of at most 0.014.
Values may be sent and summed in bfloat16 or wider, within the bound.
A program may use at most 64 MiB of HBM per device.

```python
import math
import jax
import jax.numpy as jnp
from jax import lax

D = 1280
HID = 5120
M = 256
EXPERTS = 128
IMAGES = 256


def image_tokens(base, index):
    image_key = jax.random.fold_in(base, index)
    values = jnp.clip(jax.random.normal(jax.random.fold_in(image_key, 1), (M, D), jnp.float32), -6.0, 6.0)
    return values


def draw_tokens(key, part):
    base = jax.random.fold_in(key, 11)
    stacked = jax.vmap(lambda index: image_tokens(base, index))(jnp.arange(IMAGES))
    return stacked.astype(jnp.bfloat16)


def draw_router(key, part):
    values = jax.random.normal(jax.random.fold_in(key, 12), (D, EXPERTS), jnp.float32) * (2.5 / math.sqrt(D))
    values = jnp.clip(values, -0.5, 0.5)
    return values.astype(jnp.bfloat16)


def shard_levels(key, dims, cuts, low, top_value):
    def one(dim, parts):
        draws = jax.random.uniform(jax.random.fold_in(jax.random.fold_in(key, 6), dim), (parts,), jnp.float32, low / len(cuts), top_value / len(cuts))
        return jnp.repeat(jnp.exp(draws), dims[dim] // parts).reshape((-1,) + (1,) * (len(dims) - dim - 1))

    gain = one(*cuts[0])
    for cut in cuts[1:]:
        gain = gain * one(*cut)
    return gain


def bell_draw(stream_key, dims, deviation, reach, cuts=(), dtype=jnp.bfloat16):
    factor_of = shard_levels(stream_key, dims, cuts, -0.22, 0.18) if cuts else 1.0
    array = jax.random.normal(stream_key, dims, jnp.float32) * deviation * factor_of
    return jnp.minimum(jnp.maximum(array, -reach), reach).astype(dtype)


def setup_inputs(seed: int = 0) -> dict:
    splits = jax.random.split(jax.random.key(seed), 7)
    tokens = draw_tokens(jax.random.fold_in(splits[6], 71), 0)
    router = draw_router(jax.random.fold_in(splits[6], 71), 0)
    w_in = bell_draw(splits[2], (EXPERTS, D, HID), D ** -0.5, 0.15625, ((0, 128), (2, 2)))
    b_in = bell_draw(splits[3], (EXPERTS, HID), 0.5, 3.0, ((0, 128),))
    w_out = bell_draw(splits[4], (EXPERTS, HID, D), HID ** -0.5, 0.078125, ((0, 128), (1, 2)))
    b_out = bell_draw(splits[5], (EXPERTS, D), 0.5, 3.0, ((0, 128),))
    return {"tokens": tokens, "router": router, "w_in": w_in, "b_in": b_in, "w_out": w_out, "b_out": b_out}


def run_expert(packed):
    slot_rows, weight_in, bias_in, weight_out, bias_out = packed
    hidden = jax.nn.gelu(jnp.dot(slot_rows, weight_in, preferred_element_type=jnp.float32) + bias_in.astype(jnp.float32), approximate=False).astype(jnp.bfloat16)
    return (jnp.dot(hidden, weight_out, preferred_element_type=jnp.float32) + bias_out.astype(jnp.float32)).astype(jnp.bfloat16)


def reference(tokens, router, w_in, b_in, w_out, b_out):
    logits = jnp.einsum("bmd,de->bme", tokens.astype(jnp.float32), router.astype(jnp.float32))
    dispatch = jax.nn.softmax(logits, axis=1).astype(jnp.bfloat16)
    combine = jax.nn.softmax(logits, axis=2).astype(jnp.bfloat16)
    slots = jnp.einsum("bme,bmd->ebd", dispatch.astype(jnp.float32), tokens.astype(jnp.float32)).astype(jnp.bfloat16)
    expert_out = lax.map(run_expert, (slots, w_in, b_in, w_out, b_out))
    mixed = jnp.einsum("bme,ebd->bmd", combine.astype(jnp.float32), expert_out.astype(jnp.float32))
    return mixed.astype(jnp.bfloat16)
```

```python
import functools

import jax
import jax.numpy as jnp
from jax import lax
from jax.experimental import pallas as pl
from jax.experimental.pallas import tpu as pltpu
from jax.sharding import PartitionSpec as P

MESH = pl.DeviceIdType.MESH
LANES = 128
PITCH = 16
NY, NZ, QUAD = 4, 8, 4
NQ = NY * QUAD
NP = 2 * NQ
SENDS_ORDER = (4, 3, 5, 2, 6, 1, 7)
FORWARD_ORDER = (0, 4, 3, 5, 2, 6, 1, 7)
REDUCE_ORDER = (4, 3, 5, 2, 6, 1, 7, 0)


def gelu(v):
    return v * (1.0 + lax.erf(v * (0.5**0.5))) * 0.5


def wait_copy(ref, sem):
    pltpu.make_async_copy(ref, ref, sem).wait()


def kernel(
    tokens_hbm,
    router_hbm,
    w_in_hbm,
    b_in_hbm,
    w_out_hbm,
    b_out_hbm,
    comb_ref,
    eo,
    tok,
    router,
    w_in,
    b_in,
    w_out,
    b_out,
    permuted,
    send1,
    zland,
    wide16,
    fwd,
    recv1,
    wide32,
    x_ref,
    hid,
    wide_rows,
    send2,
    recv2,
    total,
    eland,
    load_sems,
    w_in_sems,
    w_out_sems,
    send_sems,
    z_sems,
    plane1_sems,
    plane2_sems,
    eo_sem,
):
    me_dp = lax.axis_index("dp")
    me_ex = lax.axis_index("expert")
    me_y = me_ex // (NZ * QUAD)
    me_z = lax.rem(me_ex // QUAD, NZ)
    me_quad = lax.rem(me_ex, QUAD)
    me_xh, me_core = me_quad // 2, lax.rem(me_quad, 2)
    me_q = me_y * QUAD + me_quad
    me_p = me_dp * NQ + me_q
    width = tok.shape[1]
    chunks = width // LANES

    def along_z(d):
        z = lax.rem(me_z + d, NZ)
        return z, (me_dp, me_y * (NZ * QUAD) + z * QUAD + me_quad)

    ys = [lax.rem(me_y + dy, NY) for dy in range(NY)]
    quads = [lax.rem(me_xh + dx, 2) * 2 + lax.rem(me_core + dc, 2) for dc in range(2) for dx in range(2)]
    dps = [me_dp, 1 - me_dp]
    plane = []
    for t in range(NP - 1, 0, -1):
        y, a, quad = ys[t % NY], dps[t // NY % 2], quads[t // (2 * NY)]
        plane.append((a, y * QUAD + quad, (a, y * (NZ * QUAD) + me_z * QUAD + quad)))

    def each_in_plane(action):
        for target in plane:
            action(*target)

    def remote(src, dst, send_sem, recv_sem, device):
        pltpu.make_async_remote_copy(
            src_ref=src,
            dst_ref=dst,
            send_sem=send_sem,
            recv_sem=recv_sem,
            device_id=device,
            device_id_type=MESH,
        ).start()

    loads = [
        pltpu.make_async_copy(tokens_hbm.at[0], tok, load_sems.at[0]),
        pltpu.make_async_copy(router_hbm, router, load_sems.at[1]),
        pltpu.make_async_copy(b_in_hbm, b_in, load_sems.at[2]),
        pltpu.make_async_copy(b_out_hbm, b_out, load_sems.at[3]),
    ]
    loads[0].start()
    loads[1].start()
    barrier = pltpu.get_barrier_semaphore()

    def greet(device):
        pl.semaphore_signal(barrier, inc=1, device_id=device, device_id_type=MESH)

    with jax.named_scope("greet"):
        for d in SENDS_ORDER:
            greet(along_z(d)[1])
        each_in_plane(lambda a, q, device: greet(device))

    def pieces(hbm, vmem, sems):
        count = sems.shape[0]
        rows = vmem.shape[0] // count
        return [
            pltpu.make_async_copy(
                hbm.at[0, pl.ds(i * rows, rows)], vmem.at[pl.ds(i * rows, rows)], sems.at[i]
            )
            for i in range(count)
        ]

    w_in_loads = pieces(w_in_hbm, w_in, w_in_sems)
    w_out_loads = pieces(w_out_hbm, w_out, w_out_sems)
    for load in w_in_loads + loads[2:] + w_out_loads:
        load.start()

    with jax.named_scope("waittok"):
        loads[0].wait()
        loads[1].wait()
    with jax.named_scope("dispatch"):
        logits = jnp.dot(tok[...], router[...], preferred_element_type=jnp.float32).T
        for y in range(NY):
            for z in range(NZ):
                at = (y * NZ + z) * QUAD
                permuted[z * NQ + y * QUAD : z * NQ + (y + 1) * QUAD, :] = logits[at : at + QUAD, :]
        logits = permuted[...]
        over_tokens = jnp.exp(logits - jnp.max(logits, axis=1, keepdims=True))
        dispatch = (over_tokens / jnp.sum(over_tokens, axis=1, keepdims=True)).astype(jnp.bfloat16)
        send1[...] = jnp.dot(dispatch, tok[...], preferred_element_type=jnp.float32).astype(jnp.bfloat16)

    with jax.named_scope("barwait"):
        pl.semaphore_wait(barrier, NZ - 1 + NP - 1)

    with jax.named_scope("sendz"):
        for d in SENDS_ORDER:
            z, device = along_z(d)
            back = NZ - d
            remote(
                send1.at[pl.ds(pl.multiple_of(z * NQ, NQ), NQ)],
                zland.at[back],
                send_sems.at[0],
                z_sems.at[back],
                device,
            )

    def forward(r):
        if r == 0:
            block = send1[pl.ds(pl.multiple_of(me_z * NQ, NQ), NQ), :]
        else:
            wait_copy(zland.at[r], z_sems.at[r])
            block = zland[r]
        for j in range(chunks):
            wide16[r, pl.ds(j, NQ, stride=PITCH), :] = block[:, j * LANES : (j + 1) * LANES].astype(jnp.float32)
        fwd[r] = wide16[r].reshape(NQ, PITCH, LANES).astype(jnp.bfloat16)

        def send(a, q, device):
            remote(
                fwd.at[r, q, pl.ds(0, chunks)],
                recv1.at[r, me_p, pl.ds(0, chunks)],
                send_sems.at[1],
                plane1_sems.at[r],
                device,
            )

        each_in_plane(send)
        recv1[r, me_p] = fwd[r, me_q]

    with jax.named_scope("combine"):
        over_experts = jnp.exp(logits - jnp.max(logits, axis=0, keepdims=True))
        combine = over_experts / jnp.sum(over_experts, axis=0, keepdims=True)
        comb_ref[...] = combine.T.astype(jnp.bfloat16)

    for r in FORWARD_ORDER:
        with jax.named_scope("forward%d" % r):
            forward(r)

    for r in FORWARD_ORDER:
        with jax.named_scope("recv1_%d" % r):
            wait_copy(recv1.at[r, pl.ds(0, NP - 1), pl.ds(0, chunks)], plane1_sems.at[r])
            wide32[...] = recv1[r].astype(jnp.float32).reshape(wide32.shape)
            for j in range(chunks):
                x_ref[r * NP : (r + 1) * NP, j * LANES : (j + 1) * LANES] = wide32[
                    pl.ds(j, NP, stride=PITCH), :
                ].astype(jnp.bfloat16)

    for load in loads[2:] + w_in_loads:
        load.wait()
    half = w_in.shape[1]
    tile = 2 * LANES

    with jax.named_scope("mlp1"):
        for at in range(0, half, tile):
            bias = b_in[:, pl.ds(pl.multiple_of(me_dp * half + at, LANES), tile)].astype(jnp.float32)
            v = jnp.dot(x_ref[...], w_in[:, at : at + tile], preferred_element_type=jnp.float32) + bias
            hid[:, at : at + tile] = gelu(v).astype(jnp.bfloat16)

    for load in w_out_loads:
        load.wait()
    keep = (me_dp == 0).astype(jnp.float32)
    n = NZ * NP
    with jax.named_scope("mlp2"):
        for at in range(0, width, tile):
            y = jnp.dot(hid[...], w_out[:, at : at + tile], preferred_element_type=jnp.float32)
            y = y + keep * b_out[:, at : at + tile].astype(jnp.float32)
            for c in range(tile // LANES):
                wide_rows[pl.ds(at // LANES + c, n, stride=PITCH), :] = y[:, c * LANES : (c + 1) * LANES]
        send2[...] = wide_rows[...].reshape(send2.shape).astype(jnp.bfloat16)

    def scatter(r):
        def send(a, q, device):
            remote(
                send2.at[r, a * NQ + q, pl.ds(0, chunks)],
                recv2.at[r, me_p, pl.ds(0, chunks)],
                send_sems.at[2],
                plane2_sems.at[r],
                device,
            )

        each_in_plane(send)
        recv2[r, me_p] = send2[r, me_p]

    with jax.named_scope("scatter"):
        for r in REDUCE_ORDER:
            scatter(r)

    for r in REDUCE_ORDER:
        with jax.named_scope("reduce%d" % r):
            wait_copy(recv2.at[r, pl.ds(0, NP - 1), pl.ds(0, chunks)], plane2_sems.at[r])
            pair = recv2[r, :NQ].astype(jnp.float32) + recv2[r, NQ:].astype(jnp.float32)
            wide16[r] = pair.reshape(NQ * PITCH, LANES)
            for j in range(chunks):
                total[r, :, j * LANES : (j + 1) * LANES] = wide16[r, pl.ds(j, NQ, stride=PITCH), :].astype(jnp.bfloat16)
            mine = pl.ds(pl.multiple_of(me_z * NQ, NQ), NQ)
            if r == 0:
                eland[mine, :] = total[r]
            else:
                remote(total.at[r], eland.at[mine], send_sems.at[3], eo_sem, along_z(r)[1])

    with jax.named_scope("recv2"):
        wait_copy(eland.at[pl.ds(0, (NZ - 1) * NQ)], eo_sem)
    with jax.named_scope("tail"):
        eo[...] = eland[...]
        rows = recv1.at[:, pl.ds(0, NP - 1), pl.ds(0, chunks)]
        wait_copy(zland.at[pl.ds(0, NZ - 1)], send_sems.at[0])
        wait_copy(rows, send_sems.at[1])
        wait_copy(rows, send_sems.at[2])
        wait_copy(zland.at[pl.ds(0, NZ - 1)], send_sems.at[3])


def mix_kernel(combine, expert_out, out_hbm, mixed, sems):
    count = sems.shape[0]
    tile = mixed.shape[1] // count
    writes = []
    for i in range(count):
        columns = pl.ds(i * tile, tile)
        mixed[:, columns] = jnp.dot(
            combine[...], expert_out[:, columns], preferred_element_type=jnp.float32
        ).astype(mixed.dtype)
        write = pltpu.make_async_copy(mixed.at[:, columns], out_hbm.at[0, :, columns], sems.at[i])
        write.start()
        writes.append(write)
    for write in writes:
        write.wait()


def shards(tokens, router, w_in, b_in, w_out, b_out):
    images, m, width = tokens.shape
    n_ex = NZ * NQ
    n = NZ * NP
    assert images == 1 and w_in.shape[0] == 1 and router.shape[1] == n_ex
    half = w_in.shape[2]
    bf16, f32 = jnp.bfloat16, jnp.float32
    dma = pltpu.SemaphoreType.DMA
    combine, expert_out = pl.pallas_call(
        kernel,
        out_shape=[
            pltpu.VMEM((m, n_ex), bf16),
            pltpu.VMEM((n_ex, width), bf16),
        ],
        in_specs=[pl.BlockSpec(memory_space=pltpu.HBM)] * 6,
        out_specs=[pl.BlockSpec(memory_space=pltpu.VMEM)] * 2,
        scratch_shapes=[
            pltpu.VMEM((m, width), bf16),
            pltpu.VMEM(router.shape, bf16),
            pltpu.VMEM(w_in.shape[1:], bf16),
            pltpu.VMEM(b_in.shape, bf16),
            pltpu.VMEM(w_out.shape[1:], bf16),
            pltpu.VMEM(b_out.shape, bf16),
            pltpu.VMEM((n_ex, m), f32),
            pltpu.VMEM((n_ex, width), bf16),
            pltpu.VMEM((NZ, NQ, width), bf16),
            pltpu.VMEM((NZ, NQ * PITCH, LANES), f32),
            pltpu.VMEM((NZ, NQ, PITCH, LANES), bf16),
            pltpu.VMEM((NZ, NP, PITCH, LANES), bf16),
            pltpu.VMEM((NP * PITCH, LANES), f32),
            pltpu.VMEM((n, width), bf16),
            pltpu.VMEM((n, half), bf16),
            pltpu.VMEM((n * PITCH, LANES), f32),
            pltpu.VMEM((NZ, NP, PITCH, LANES), bf16),
            pltpu.VMEM((NZ, NP, PITCH, LANES), bf16),
            pltpu.VMEM((NZ, NQ, width), bf16),
            pltpu.VMEM((n_ex, width), bf16),
            dma((4,)),
            dma((4,)),
            dma((4,)),
            dma((4,)),
            dma((NZ,)),
            dma((NZ,)),
            dma((NZ,)),
            dma,
        ],
        compiler_params=pltpu.CompilerParams(
            collective_id=0, has_side_effects=True, vmem_limit_bytes=60 * 1024 * 1024
        ),
    )(tokens, router, w_in, b_in, w_out, b_out)
    tile = 2 * LANES
    return pl.pallas_call(
        mix_kernel,
        out_shape=jax.ShapeDtypeStruct(tokens.shape, bf16),
        in_specs=[pl.BlockSpec(memory_space=pltpu.VMEM)] * 2,
        out_specs=pl.BlockSpec(memory_space=pltpu.HBM),
        scratch_shapes=[
            pltpu.VMEM((m, width), bf16),
            dma((width // tile,)),
        ],
        compiler_params=pltpu.CompilerParams(vmem_limit_bytes=8 * 1024 * 1024),
    )(combine, expert_out)


def solution(mesh):
    return jax.shard_map(
        shards,
        mesh=mesh,
        in_specs=(
            P(("dp", "expert"), None, None),
            P(),
            P("expert", None, "dp"),
            P("expert", None),
            P("expert", "dp", None),
            P("expert", None),
        ),
        out_specs=P(("dp", "expert"), None, None),
        check_vma=False,
    )
```

```python
import functools

import jax
import jax.numpy as jnp
from jax import lax
from jax.experimental import pallas as pl
from jax.experimental.pallas import tpu as pltpu
from jax.sharding import PartitionSpec as P

MESH = pl.DeviceIdType.MESH
LANES = 128
PITCH = 16
NY, NZ, QUAD = 4, 8, 4
NQ = NY * QUAD
NP = 2 * NQ
COLUMN = (4, 3, 5, 2, 6, 1, 7)
FORWARD_ORDER = (0, 4, 3, 5, 2, 6, 1, 7)
BATCHES = ((0, 4, 3, 5), (2, 6, 1, 7))
SCATTERS = ((4, 3, 5), (2, 6, 1, 7, 0))
REDUCE_ORDER = (4, 3, 5, 2, 6, 0)
DIRECT = (1, 7)


def gelu(v):
    return v * (1.0 + lax.erf(v * (0.5**0.5))) * 0.5


def wait_copy(ref, sem):
    pltpu.make_async_copy(ref, ref, sem).wait()


def kernel(
    tokens_hbm,
    router_hbm,
    w_in_hbm,
    b_in_hbm,
    w_out_hbm,
    b_out_hbm,
    comb_ref,
    eo,
    tok,
    router,
    w_in,
    b_in,
    w_out,
    b_out,
    permuted,
    send1,
    zland,
    wide16,
    fwd,
    recv1,
    wide32,
    x_ref,
    hid,
    wide_rows,
    send2,
    recv2,
    total,
    eland,
    load_sems,
    w_in_sems,
    w_out_sems,
    send_sems,
    z_sems,
    plane1_sems,
    plane2_sems,
    eo_sems,
):
    me_dp = lax.axis_index("dp")
    me_ex = lax.axis_index("expert")
    me_y = me_ex // (NZ * QUAD)
    me_z = lax.rem(me_ex // QUAD, NZ)
    me_quad = lax.rem(me_ex, QUAD)
    me_xh, me_core = me_quad // 2, lax.rem(me_quad, 2)
    me_q = me_y * QUAD + me_quad
    me_p = me_dp * NQ + me_q
    width = tok.shape[1]
    chunks = width // LANES

    def along_z(d):
        z = lax.rem(me_z + d, NZ)
        return z, (me_dp, me_y * (NZ * QUAD) + z * QUAD + me_quad)

    ys = [lax.rem(me_y + dy, NY) for dy in range(NY)]
    quads = [lax.rem(me_xh + dx, 2) * 2 + lax.rem(me_core + dc, 2) for dc in range(2) for dx in range(2)]
    dps = [me_dp, 1 - me_dp]
    plane = []
    for t in range(NP - 1, -1, -1):
        y, a, quad = ys[t % NY], dps[t // NY % 2], quads[t // (2 * NY)]
        plane.append((a, y * QUAD + quad, y * (NZ * QUAD) + quad))

    def each_in_plane(d, action):
        z = lax.rem(me_z + d, NZ) * QUAD
        for a, q, ex in plane if d else plane[:-1]:
            action(a, q, (a, ex + z))

    def remote(src, dst, send_sem, recv_sem, device):
        pltpu.make_async_remote_copy(
            src_ref=src,
            dst_ref=dst,
            send_sem=send_sem,
            recv_sem=recv_sem,
            device_id=device,
            device_id_type=MESH,
        ).start()

    loads = [
        pltpu.make_async_copy(tokens_hbm.at[0], tok, load_sems.at[0]),
        pltpu.make_async_copy(router_hbm, router, load_sems.at[1]),
        pltpu.make_async_copy(b_in_hbm, b_in, load_sems.at[2]),
        pltpu.make_async_copy(b_out_hbm, b_out, load_sems.at[3]),
    ]
    loads[0].start()
    loads[1].start()
    barrier = pltpu.get_barrier_semaphore()

    def greet(device):
        pl.semaphore_signal(barrier, inc=1, device_id=device, device_id_type=MESH)

    with jax.named_scope("greet"):
        for d in COLUMN:
            greet(along_z(d)[1])
        each_in_plane(0, lambda a, q, device: greet(device))

    def pieces(hbm, vmem, sems):
        count = sems.shape[0]
        rows = vmem.shape[0] // count
        return [
            pltpu.make_async_copy(
                hbm.at[0, pl.ds(i * rows, rows)], vmem.at[pl.ds(i * rows, rows)], sems.at[i]
            )
            for i in range(count)
        ]

    w_in_loads = pieces(w_in_hbm, w_in, w_in_sems)
    w_out_loads = pieces(w_out_hbm, w_out, w_out_sems)
    for load in w_in_loads + loads[2:] + w_out_loads:
        load.start()

    with jax.named_scope("waittok"):
        loads[0].wait()
        loads[1].wait()
    with jax.named_scope("dispatch"):
        logits = jnp.dot(tok[...], router[...], preferred_element_type=jnp.float32).T
        for y in range(NY):
            for z in range(NZ):
                at = (y * NZ + z) * QUAD
                permuted[z * NQ + y * QUAD : z * NQ + (y + 1) * QUAD, :] = logits[at : at + QUAD, :]
        logits = permuted[...]
        over_tokens = jnp.exp(logits - jnp.max(logits, axis=1, keepdims=True))
        dispatch = (over_tokens / jnp.sum(over_tokens, axis=1, keepdims=True)).astype(jnp.bfloat16)
        send1[...] = jnp.dot(dispatch, tok[...], preferred_element_type=jnp.float32).astype(jnp.bfloat16)

    with jax.named_scope("barwait"):
        pl.semaphore_wait(barrier, NZ - 1 + NP - 1)

    with jax.named_scope("sendz"):
        for d in COLUMN:
            z, device = along_z(d)
            back = NZ - d
            remote(
                send1.at[pl.ds(pl.multiple_of(z * NQ, NQ), NQ)],
                zland.at[back],
                send_sems.at[0],
                z_sems.at[back],
                device,
            )

    def forward(r):
        if r == 0:
            block = send1[pl.ds(pl.multiple_of(me_z * NQ, NQ), NQ), :]
        else:
            wait_copy(zland.at[r], z_sems.at[r])
            block = zland[r]
        for j in range(chunks):
            wide16[r, pl.ds(j, NQ, stride=PITCH), :] = block[:, j * LANES : (j + 1) * LANES].astype(jnp.float32)
        fwd[r] = wide16[r].reshape(NQ, PITCH, LANES).astype(jnp.bfloat16)

        def send(a, q, device):
            remote(
                fwd.at[r, q, pl.ds(0, chunks)],
                recv1.at[r, me_p, pl.ds(0, chunks)],
                send_sems.at[1],
                plane1_sems.at[r],
                device,
            )

        each_in_plane(0, send)
        recv1[r, me_p] = fwd[r, me_q]

    with jax.named_scope("combine"):
        over_experts = jnp.exp(logits - jnp.max(logits, axis=0, keepdims=True))
        combine = over_experts / jnp.sum(over_experts, axis=0, keepdims=True)
        comb_ref[...] = combine.T.astype(jnp.bfloat16)

    for r in FORWARD_ORDER:
        with jax.named_scope("forward%d" % r):
            forward(r)

    half = w_in.shape[1]
    tile = 2 * LANES
    keep = (me_dp == 0).astype(jnp.float32)

    def gather(r, at):
        with jax.named_scope("gather%d" % r):
            wait_copy(recv1.at[r, pl.ds(0, NP - 1), pl.ds(0, chunks)], plane1_sems.at[r])
            wide32[...] = recv1[r].astype(jnp.float32).reshape(wide32.shape)
            for j in range(chunks):
                x_ref[at : at + NP, j * LANES : (j + 1) * LANES] = wide32[
                    pl.ds(j, NP, stride=PITCH), :
                ].astype(jnp.bfloat16)

    def scatter(r):
        def send(a, q, device):
            remote(
                send2.at[r, a * NQ + q, pl.ds(0, chunks)],
                recv2.at[r, me_p, pl.ds(0, chunks)],
                send_sems.at[2],
                plane2_sems.at[r],
                device,
            )

        each_in_plane(r if r in DIRECT else 0, send)

    start = 0
    for batch, leaving in zip(BATCHES, SCATTERS, strict=True):
        n = len(batch) * NP
        rows = slice(start, start + n)
        for i, r in enumerate(batch):
            gather(r, start + i * NP)
        if start == 0:
            for load in loads[2:] + w_in_loads:
                load.wait()
        with jax.named_scope("mlp1_%d" % start):
            for at in range(0, half, tile):
                bias = b_in[:, pl.ds(pl.multiple_of(me_dp * half + at, LANES), tile)].astype(jnp.float32)
                v = jnp.dot(x_ref[rows, :], w_in[:, at : at + tile], preferred_element_type=jnp.float32) + bias
                hid[rows, at : at + tile] = gelu(v).astype(jnp.bfloat16)
        if start == 0:
            for load in w_out_loads:
                load.wait()
        with jax.named_scope("mlp2_%d" % start):
            for at in range(0, width, tile):
                y = jnp.dot(hid[rows, :], w_out[:, at : at + tile], preferred_element_type=jnp.float32)
                y = y + keep * b_out[:, at : at + tile].astype(jnp.float32)
                for c in range(tile // LANES):
                    wide_rows[pl.ds(start * PITCH + at // LANES + c, n, stride=PITCH), :] = y[
                        :, c * LANES : (c + 1) * LANES
                    ]
        with jax.named_scope("scatter_%d" % start):
            for r in sorted(batch, key=(leaving + (0,)).index):
                first = (start + batch.index(r) * NP) * PITCH
                send2[r] = wide_rows[first : first + NP * PITCH, :].reshape(NP, PITCH, LANES).astype(jnp.bfloat16)
                if r not in DIRECT:
                    recv2[r, me_p] = send2[r, me_p]
            for r in leaving:
                scatter(r)
        start += n

    def reduce(r):
        rows = NP if r in DIRECT else NP - 1
        wait_copy(recv2.at[r, pl.ds(0, rows), pl.ds(0, chunks)], plane2_sems.at[r])
        pair = recv2[r, :NQ].astype(jnp.float32) + recv2[r, NQ:].astype(jnp.float32)
        wide16[r] = pair.reshape(NQ * PITCH, LANES)
        for j in range(chunks):
            total[r, :, j * LANES : (j + 1) * LANES] = wide16[r, pl.ds(j, NQ, stride=PITCH), :].astype(jnp.bfloat16)

    def expert_rows(z):
        return pl.ds(pl.multiple_of(z * NQ, NQ), NQ)

    for r in REDUCE_ORDER:
        with jax.named_scope("reduce%d" % r):
            reduce(r)
            if r == 0:
                eland[0] = total[0]
            else:
                remote(total.at[r], eland.at[NZ - r], send_sems.at[3], eo_sems.at[NZ - r], along_z(r)[1])
    for r in DIRECT:
        with jax.named_scope("direct%d" % r):
            reduce(r)
            eland[NZ - r] = total[r]

    for r in (4, 3, 5, 2, 6, 1, 7, 0):
        with jax.named_scope("eo%d" % r):
            back = (NZ - r) % NZ
            if r and r not in DIRECT:
                wait_copy(eland.at[back], eo_sems.at[back])
            eo[expert_rows(lax.rem(me_z + back, NZ)), :] = eland[back]
    with jax.named_scope("tail"):
        sent = recv1.at[:, pl.ds(0, NP - 1), pl.ds(0, chunks)]
        wait_copy(sent, send_sems.at[1])
        wait_copy(sent, send_sems.at[2])
        for r in DIRECT:
            wait_copy(recv1.at[r, 0, pl.ds(0, chunks)], send_sems.at[2])
        wait_copy(zland.at[pl.ds(0, NZ - 1)], send_sems.at[0])
        wait_copy(zland.at[pl.ds(0, len(REDUCE_ORDER) - 1)], send_sems.at[3])


def mix_kernel(combine, expert_out, out_hbm, mixed, sems):
    count = sems.shape[0]
    tile = mixed.shape[1] // count
    writes = []
    for i in range(count):
        columns = pl.ds(i * tile, tile)
        mixed[:, columns] = jnp.dot(
            combine[...], expert_out[:, columns], preferred_element_type=jnp.float32
        ).astype(mixed.dtype)
        write = pltpu.make_async_copy(mixed.at[:, columns], out_hbm.at[0, :, columns], sems.at[i])
        write.start()
        writes.append(write)
    for write in writes:
        write.wait()


def shards(tokens, router, w_in, b_in, w_out, b_out):
    images, m, width = tokens.shape
    n_ex = NZ * NQ
    n = NZ * NP
    assert images == 1 and w_in.shape[0] == 1 and router.shape[1] == n_ex
    half = w_in.shape[2]
    bf16, f32 = jnp.bfloat16, jnp.float32
    dma = pltpu.SemaphoreType.DMA
    combine, expert_out = pl.pallas_call(
        kernel,
        out_shape=[
            pltpu.VMEM((m, n_ex), bf16),
            pltpu.VMEM((n_ex, width), bf16),
        ],
        in_specs=[pl.BlockSpec(memory_space=pltpu.HBM)] * 6,
        out_specs=[pl.BlockSpec(memory_space=pltpu.VMEM)] * 2,
        scratch_shapes=[
            pltpu.VMEM((m, width), bf16),
            pltpu.VMEM(router.shape, bf16),
            pltpu.VMEM(w_in.shape[1:], bf16),
            pltpu.VMEM(b_in.shape, bf16),
            pltpu.VMEM(w_out.shape[1:], bf16),
            pltpu.VMEM(b_out.shape, bf16),
            pltpu.VMEM((n_ex, m), f32),
            pltpu.VMEM((n_ex, width), bf16),
            pltpu.VMEM((NZ, NQ, width), bf16),
            pltpu.VMEM((NZ, NQ * PITCH, LANES), f32),
            pltpu.VMEM((NZ, NQ, PITCH, LANES), bf16),
            pltpu.VMEM((NZ, NP, PITCH, LANES), bf16),
            pltpu.VMEM((NP * PITCH, LANES), f32),
            pltpu.VMEM((n, width), bf16),
            pltpu.VMEM((n, half), bf16),
            pltpu.VMEM((n * PITCH, LANES), f32),
            pltpu.VMEM((NZ, NP, PITCH, LANES), bf16),
            pltpu.VMEM((NZ, NP, PITCH, LANES), bf16),
            pltpu.VMEM((NZ, NQ, width), bf16),
            pltpu.VMEM((NZ, NQ, width), bf16),
            dma((4,)),
            dma((4,)),
            dma((4,)),
            dma((4,)),
            dma((NZ,)),
            dma((NZ,)),
            dma((NZ,)),
            dma((NZ,)),
        ],
        compiler_params=pltpu.CompilerParams(
            collective_id=0, has_side_effects=True, vmem_limit_bytes=60 * 1024 * 1024
        ),
    )(tokens, router, w_in, b_in, w_out, b_out)
    tile = 2 * LANES
    return pl.pallas_call(
        mix_kernel,
        out_shape=jax.ShapeDtypeStruct(tokens.shape, bf16),
        in_specs=[pl.BlockSpec(memory_space=pltpu.VMEM)] * 2,
        out_specs=pl.BlockSpec(memory_space=pltpu.HBM),
        scratch_shapes=[
            pltpu.VMEM((m, width), bf16),
            dma((width // tile,)),
        ],
        compiler_params=pltpu.CompilerParams(vmem_limit_bytes=8 * 1024 * 1024),
    )(combine, expert_out)


def solution(mesh):
    return jax.shard_map(
        shards,
        mesh=mesh,
        in_specs=(
            P(("dp", "expert"), None, None),
            P(),
            P("expert", None, "dp"),
            P("expert", None),
            P("expert", "dp", None),
            P("expert", None),
        ),
        out_specs=P(("dp", "expert"), None, None),
        check_vma=False,
    )
```

```python
import functools

import jax
import jax.numpy as jnp
from jax import lax
from jax.experimental import pallas as pl
from jax.experimental.pallas import tpu as pltpu
from jax.sharding import PartitionSpec as P

MESH = pl.DeviceIdType.MESH
LANES = 128
PITCH = 16
NY, NZ, QUAD = 4, 8, 4
NQ = NY * QUAD
NP = 2 * NQ
COLUMN = (4, 1, 7, 2, 6, 3, 5)
BATCHES = ((0, 4, 1, 7), (3, 5, 2, 6))
DIRECT = ()
STEPS = "f0 f4 f1 f7 f2 f6 f3 f5 g0 g4 g1 g7 m0 s4 s1 s7 g3 g5 g2 g6 m1 s3 s5 r4 r1 r7 s2 s6 s0 r3 r5 r2 r6 r0".split()


def gelu(v):
    return v * (1.0 + lax.erf(v * (0.5**0.5))) * 0.5


def wait_copy(ref, sem):
    pltpu.make_async_copy(ref, ref, sem).wait()


def kernel(
    tokens_hbm,
    router_hbm,
    w_in_hbm,
    b_in_hbm,
    w_out_hbm,
    b_out_hbm,
    comb_ref,
    eo,
    tok,
    router,
    w_in,
    b_in,
    w_out,
    b_out,
    permuted,
    send1,
    zland,
    wide16,
    fwd,
    recv1,
    wide32,
    x_ref,
    hid,
    wide_rows,
    send2,
    recv2,
    total,
    eland,
    load_sems,
    send_sem,
    z_sems,
    plane1_sems,
    plane2_sems,
    eo_sem,
):
    me_dp = lax.axis_index("dp")
    me_ex = lax.axis_index("expert")
    me_y = me_ex // (NZ * QUAD)
    me_z = lax.rem(me_ex // QUAD, NZ)
    me_quad = lax.rem(me_ex, QUAD)
    me_xh, me_core = me_quad // 2, lax.rem(me_quad, 2)
    me_q = me_y * QUAD + me_quad
    me_p = me_dp * NQ + me_q
    width = tok.shape[1]
    chunks = width // LANES

    def along_z(d):
        z = lax.rem(me_z + d, NZ)
        return z, (me_dp, me_y * (NZ * QUAD) + z * QUAD + me_quad)

    ys = [lax.rem(me_y + dy, NY) for dy in range(NY)]
    quads = [lax.rem(me_xh + dx, 2) * 2 + lax.rem(me_core + dc, 2) for dc in range(2) for dx in range(2)]
    dps = [me_dp, 1 - me_dp]
    plane = []
    for t in range(NP - 1, -1, -1):
        y, a, quad = ys[t % NY], dps[t // NY % 2], quads[t // (2 * NY)]
        plane.append((a, y * QUAD + quad, y * (NZ * QUAD) + quad))

    def each_in_plane(d, action):
        z = lax.rem(me_z + d, NZ) * QUAD
        for a, q, ex in plane if d else plane[:-1]:
            action(a, q, (a, ex + z))

    def remote(src, dst, send_sem, recv_sem, device):
        pltpu.make_async_remote_copy(
            src_ref=src,
            dst_ref=dst,
            send_sem=send_sem,
            recv_sem=recv_sem,
            device_id=device,
            device_id_type=MESH,
        ).start()

    loads = [
        pltpu.make_async_copy(tokens_hbm.at[0], tok, load_sems.at[0]),
        pltpu.make_async_copy(router_hbm, router, load_sems.at[0]),
        pltpu.make_async_copy(w_in_hbm.at[0], w_in, load_sems.at[1]),
        pltpu.make_async_copy(b_in_hbm, b_in, load_sems.at[1]),
        pltpu.make_async_copy(w_out_hbm.at[0], w_out, load_sems.at[1]),
        pltpu.make_async_copy(b_out_hbm, b_out, load_sems.at[1]),
    ]
    loads[0].start()
    loads[1].start()
    barrier = pltpu.get_barrier_semaphore()

    def greet(device):
        pl.semaphore_signal(barrier, inc=1, device_id=device, device_id_type=MESH)

    with jax.named_scope("greet"):
        for d in COLUMN:
            greet(along_z(d)[1])
        each_in_plane(0, lambda a, q, device: greet(device))

    for load in loads[2:]:
        load.start()

    with jax.named_scope("waittok"):
        loads[0].wait()
        loads[1].wait()
    with jax.named_scope("dispatch"):
        logits = jnp.dot(tok[...], router[...], preferred_element_type=jnp.float32).T
        for y in range(NY):
            for z in range(NZ):
                at = (y * NZ + z) * QUAD
                permuted[z * NQ + y * QUAD : z * NQ + (y + 1) * QUAD, :] = logits[at : at + QUAD, :]
        logits = permuted[...]
        over_tokens = jnp.exp(logits - jnp.max(logits, axis=1, keepdims=True))
        dispatch = (over_tokens / jnp.sum(over_tokens, axis=1, keepdims=True)).astype(jnp.bfloat16)
        send1[...] = jnp.dot(dispatch, tok[...], preferred_element_type=jnp.float32).astype(jnp.bfloat16)

    with jax.named_scope("barwait"):
        pl.semaphore_wait(barrier, NZ - 1 + NP - 1)

    with jax.named_scope("sendz"):
        for d in COLUMN:
            z, device = along_z(d)
            back = NZ - d
            remote(
                send1.at[pl.ds(pl.multiple_of(z * NQ, NQ), NQ)],
                zland.at[back],
                send_sem,
                z_sems.at[back],
                device,
            )

    def forward(r):
        if r == 0:
            block = send1[pl.ds(pl.multiple_of(me_z * NQ, NQ), NQ), :]
        else:
            wait_copy(zland.at[r], z_sems.at[r])
            block = zland[r]
        for j in range(chunks):
            wide16[r, pl.ds(j, NQ, stride=PITCH), :] = block[:, j * LANES : (j + 1) * LANES].astype(jnp.float32)
        fwd[r] = wide16[r].reshape(NQ, PITCH, LANES).astype(jnp.bfloat16)

        def send(a, q, device):
            remote(
                fwd.at[r, q, pl.ds(0, chunks)],
                recv1.at[r, me_p, pl.ds(0, chunks)],
                send_sem,
                plane1_sems.at[r],
                device,
            )

        each_in_plane(0, send)
        recv1[r, me_p] = fwd[r, me_q]

    with jax.named_scope("combine"):
        over_experts = jnp.exp(logits - jnp.max(logits, axis=0, keepdims=True))
        combine = over_experts / jnp.sum(over_experts, axis=0, keepdims=True)
        comb_ref[...] = combine.T.astype(jnp.bfloat16)

    half = w_in.shape[1]
    tile = 2 * LANES
    keep = (me_dp == 0).astype(jnp.float32)

    def gather(r):
        at = order.index(r) * NP
        wait_copy(recv1.at[r, pl.ds(0, NP - 1), pl.ds(0, chunks)], plane1_sems.at[r])
        wide32[...] = recv1[r].astype(jnp.float32).reshape(wide32.shape)
        for j in range(chunks):
            x_ref[at : at + NP, j * LANES : (j + 1) * LANES] = wide32[
                pl.ds(j, NP, stride=PITCH), :
            ].astype(jnp.bfloat16)

    def multiply(batch):
        start = order.index(BATCHES[batch][0]) * NP
        n = len(BATCHES[batch]) * NP
        rows = slice(start, start + n)
        if batch == 0:
            for load in loads[2:]:
                load.wait()
        for at in range(0, half, tile):
            bias = b_in[:, pl.ds(pl.multiple_of(me_dp * half + at, LANES), tile)].astype(jnp.float32)
            v = jnp.dot(x_ref[rows, :], w_in[:, at : at + tile], preferred_element_type=jnp.float32) + bias
            hid[rows, at : at + tile] = gelu(v).astype(jnp.bfloat16)
        for at in range(0, width, tile):
            y = jnp.dot(hid[rows, :], w_out[:, at : at + tile], preferred_element_type=jnp.float32)
            y = y + keep * b_out[:, at : at + tile].astype(jnp.float32)
            for c in range(tile // LANES):
                wide_rows[pl.ds(start * PITCH + at // LANES + c, n, stride=PITCH), :] = y[
                    :, c * LANES : (c + 1) * LANES
                ]
        for r in BATCHES[batch]:
            first = order.index(r) * NP * PITCH
            send2[r] = wide_rows[first : first + NP * PITCH, :].reshape(NP, PITCH, LANES).astype(jnp.bfloat16)

    def scatter(r):
        def send(a, q, device):
            remote(
                send2.at[r, a * NQ + q, pl.ds(0, chunks)],
                recv2.at[r, me_p, pl.ds(0, chunks)],
                send_sem,
                plane2_sems.at[r],
                device,
            )

        each_in_plane(r if r in DIRECT else 0, send)
        if r not in DIRECT:
            recv2[r, me_p] = send2[r, me_p]

    def reduce(r):
        rows = NP if r in DIRECT else NP - 1
        wait_copy(recv2.at[r, pl.ds(0, rows), pl.ds(0, chunks)], plane2_sems.at[r])
        pair = recv2[r, :NQ].astype(jnp.float32) + recv2[r, NQ:].astype(jnp.float32)
        wide16[r] = pair.reshape(NQ * PITCH, LANES)
        for j in range(chunks):
            total[r, :, j * LANES : (j + 1) * LANES] = wide16[r, pl.ds(j, NQ, stride=PITCH), :].astype(jnp.bfloat16)
        back = (NZ - r) % NZ
        if r == 0 or r in DIRECT:
            eo[expert_rows(back), :] = total[r]
        else:
            remote(total.at[r], eland.at[back], send_sem, eo_sem, along_z(r)[1])

    def expert_rows(d):
        return pl.ds(pl.multiple_of(lax.rem(me_z + d, NZ) * NQ, NQ), NQ)

    order = sum(BATCHES, ())
    actions = {"f": forward, "g": gather, "m": multiply, "s": scatter, "r": reduce}
    for step in STEPS:
        with jax.named_scope(step):
            actions[step[0]](int(step[1]))

    relayed = [r for r in COLUMN if r not in DIRECT]
    with jax.named_scope("eo"):
        wait_copy(zland.at[pl.ds(0, len(relayed))], eo_sem)
        for r in relayed:
            eo[expert_rows(NZ - r), :] = eland[NZ - r]
    with jax.named_scope("tail"):
        for sent in (recv1, recv2):
            wait_copy(sent.at[:, pl.ds(0, NP - 1), pl.ds(0, chunks)], send_sem)
        for r in DIRECT:
            wait_copy(recv1.at[r, 0, pl.ds(0, chunks)], send_sem)
        wait_copy(zland.at[pl.ds(0, NZ - 1)], send_sem)
        wait_copy(zland.at[pl.ds(0, len(relayed))], send_sem)


def mix_kernel(combine, expert_out, out_hbm, mixed, sems):
    count = sems.shape[0]
    tile = mixed.shape[1] // count
    writes = []
    for i in range(count):
        columns = pl.ds(i * tile, tile)
        mixed[:, columns] = jnp.dot(
            combine[...], expert_out[:, columns], preferred_element_type=jnp.float32
        ).astype(mixed.dtype)
        write = pltpu.make_async_copy(mixed.at[:, columns], out_hbm.at[0, :, columns], sems.at[i])
        write.start()
        writes.append(write)
    for write in writes:
        write.wait()


def shards(tokens, router, w_in, b_in, w_out, b_out):
    images, m, width = tokens.shape
    n_ex = NZ * NQ
    n = NZ * NP
    assert images == 1 and w_in.shape[0] == 1 and router.shape[1] == n_ex
    half = w_in.shape[2]
    bf16, f32 = jnp.bfloat16, jnp.float32
    dma = pltpu.SemaphoreType.DMA
    combine, expert_out = pl.pallas_call(
        kernel,
        out_shape=[
            pltpu.VMEM((m, n_ex), bf16),
            pltpu.VMEM((n_ex, width), bf16),
        ],
        in_specs=[pl.BlockSpec(memory_space=pltpu.HBM)] * 6,
        out_specs=[pl.BlockSpec(memory_space=pltpu.VMEM)] * 2,
        scratch_shapes=[
            pltpu.VMEM((m, width), bf16),
            pltpu.VMEM(router.shape, bf16),
            pltpu.VMEM(w_in.shape[1:], bf16),
            pltpu.VMEM(b_in.shape, bf16),
            pltpu.VMEM(w_out.shape[1:], bf16),
            pltpu.VMEM(b_out.shape, bf16),
            pltpu.VMEM((n_ex, m), f32),
            pltpu.VMEM((n_ex, width), bf16),
            pltpu.VMEM((NZ, NQ, width), bf16),
            pltpu.VMEM((NZ, NQ * PITCH, LANES), f32),
            pltpu.VMEM((NZ, NQ, PITCH, LANES), bf16),
            pltpu.VMEM((NZ, NP, PITCH, LANES), bf16),
            pltpu.VMEM((NP * PITCH, LANES), f32),
            pltpu.VMEM((n, width), bf16),
            pltpu.VMEM((n, half), bf16),
            pltpu.VMEM((n * PITCH, LANES), f32),
            pltpu.VMEM((NZ, NP, PITCH, LANES), bf16),
            pltpu.VMEM((NZ, NP, PITCH, LANES), bf16),
            pltpu.VMEM((NZ, NQ, width), bf16),
            pltpu.VMEM((NZ, NQ, width), bf16),
            dma((2,)),
            dma,
            dma((NZ,)),
            dma((NZ,)),
            dma((NZ,)),
            dma,
        ],
        compiler_params=pltpu.CompilerParams(
            collective_id=0, has_side_effects=True, vmem_limit_bytes=60 * 1024 * 1024
        ),
    )(tokens, router, w_in, b_in, w_out, b_out)
    tile = 2 * LANES
    return pl.pallas_call(
        mix_kernel,
        out_shape=jax.ShapeDtypeStruct(tokens.shape, bf16),
        in_specs=[pl.BlockSpec(memory_space=pltpu.VMEM)] * 2,
        out_specs=pl.BlockSpec(memory_space=pltpu.HBM),
        scratch_shapes=[
            pltpu.VMEM((m, width), bf16),
            dma((width // tile,)),
        ],
        compiler_params=pltpu.CompilerParams(vmem_limit_bytes=8 * 1024 * 1024),
    )(combine, expert_out)


def solution(mesh):
    return jax.shard_map(
        shards,
        mesh=mesh,
        in_specs=(
            P(("dp", "expert"), None, None),
            P(),
            P("expert", None, "dp"),
            P("expert", None),
            P("expert", "dp", None),
            P("expert", None),
        ),
        out_specs=P(("dp", "expert"), None, None),
        check_vma=False,
    )
```

```python
import functools

import jax
import jax.numpy as jnp
from jax import lax
from jax.experimental import pallas as pl
from jax.experimental.pallas import tpu as pltpu
from jax.sharding import PartitionSpec as P

MESH = pl.DeviceIdType.MESH
LANES = 128
PITCH = 16
NY, NZ, QUAD = 4, 8, 4
NQ = NY * QUAD
NP = 2 * NQ
COLUMN = (4, 1, 7, 2, 6, 3, 5)
BATCHES = ((0, 4, 1, 7), (3, 5, 2, 6))
DIRECT = ()
STEPS = ("f0", "f4", "f1", "f7", "f2", "f6", "f3", "f5", "g0", "g4", "g1", "g7", "m0", "s4", "s1", "s7", "g3", "g5", "g2", "g6", "m1", "s3", "s5", "r4", "r1", "r7", "s2", "s6", "s0", "r3", "r5", "r2", "r6", "r0")
TILE1 = 256
TILE2 = 256


def gelu(v):
    return v * (1.0 + lax.erf(v * (0.5**0.5))) * 0.5


def wait_copy(ref, sem):
    pltpu.make_async_copy(ref, ref, sem).wait()


def kernel(
    tokens_hbm,
    router_hbm,
    w_in_hbm,
    b_in_hbm,
    w_out_hbm,
    b_out_hbm,
    comb_ref,
    eo,
    tok,
    router,
    w_in,
    b_in,
    w_out,
    b_out,
    permuted,
    send1,
    zland,
    wide16,
    fwd,
    recv1,
    wide32,
    x_ref,
    hid,
    wide_rows,
    send2,
    recv2,
    total,
    eland,
    load_sems,
    send_sem,
    z_sems,
    plane1_sems,
    plane2_sems,
    eo_sem,
):
    me_dp = lax.axis_index("dp")
    me_ex = lax.axis_index("expert")
    me_y = me_ex // (NZ * QUAD)
    me_z = lax.rem(me_ex // QUAD, NZ)
    me_quad = lax.rem(me_ex, QUAD)
    me_xh, me_core = me_quad // 2, lax.rem(me_quad, 2)
    me_q = me_y * QUAD + me_quad
    me_p = me_dp * NQ + me_q
    width = tok.shape[1]
    chunks = width // LANES

    def along_z(d):
        z = lax.rem(me_z + d, NZ)
        return z, (me_dp, me_y * (NZ * QUAD) + z * QUAD + me_quad)

    ys = [lax.rem(me_y + dy, NY) for dy in range(NY)]
    quads = [lax.rem(me_xh + dx, 2) * 2 + lax.rem(me_core + dc, 2) for dc in range(2) for dx in range(2)]
    dps = [me_dp, 1 - me_dp]
    plane = []
    for t in range(NP - 1, -1, -1):
        y, a, quad = ys[t % NY], dps[t // NY % 2], quads[t // (2 * NY)]
        plane.append((a, y * QUAD + quad, y * (NZ * QUAD) + quad))

    def each_in_plane(d, action):
        z = lax.rem(me_z + d, NZ) * QUAD
        for a, q, ex in plane if d else plane[:-1]:
            action(a, q, (a, ex + z))

    def remote(src, dst, send_sem, recv_sem, device):
        pltpu.make_async_remote_copy(
            src_ref=src,
            dst_ref=dst,
            send_sem=send_sem,
            recv_sem=recv_sem,
            device_id=device,
            device_id_type=MESH,
        ).start()

    loads = [
        pltpu.make_async_copy(tokens_hbm.at[0], tok, load_sems.at[0]),
        pltpu.make_async_copy(router_hbm, router, load_sems.at[0]),
        pltpu.make_async_copy(w_in_hbm.at[0], w_in, load_sems.at[1]),
        pltpu.make_async_copy(b_in_hbm, b_in, load_sems.at[1]),
        pltpu.make_async_copy(w_out_hbm.at[0], w_out, load_sems.at[1]),
        pltpu.make_async_copy(b_out_hbm, b_out, load_sems.at[1]),
    ]
    loads[0].start()
    loads[1].start()
    barrier = pltpu.get_barrier_semaphore()

    def greet(device):
        pl.semaphore_signal(barrier, inc=1, device_id=device, device_id_type=MESH)

    with jax.named_scope("greet"):
        for d in COLUMN:
            greet(along_z(d)[1])
        each_in_plane(0, lambda a, q, device: greet(device))

    for load in loads[2:]:
        load.start()

    with jax.named_scope("waittok"):
        loads[0].wait()
        loads[1].wait()
    with jax.named_scope("dispatch"):
        logits = jnp.dot(tok[...], router[...], preferred_element_type=jnp.float32).T
        for y in range(NY):
            for z in range(NZ):
                at = (y * NZ + z) * QUAD
                permuted[z * NQ + y * QUAD : z * NQ + (y + 1) * QUAD, :] = logits[at : at + QUAD, :]
        logits = permuted[...]
        over_tokens = jnp.exp(logits - jnp.max(logits, axis=1, keepdims=True))
        dispatch = (over_tokens / jnp.sum(over_tokens, axis=1, keepdims=True)).astype(jnp.bfloat16)
        send1[...] = jnp.dot(dispatch, tok[...], preferred_element_type=jnp.float32).astype(jnp.bfloat16)

    with jax.named_scope("barwait"):
        pl.semaphore_wait(barrier, NZ - 1 + NP - 1)

    with jax.named_scope("sendz"):
        for d in COLUMN:
            z, device = along_z(d)
            back = NZ - d
            remote(
                send1.at[pl.ds(pl.multiple_of(z * NQ, NQ), NQ)],
                zland.at[back],
                send_sem,
                z_sems.at[back],
                device,
            )

    def forward(r):
        if r == 0:
            block = send1[pl.ds(pl.multiple_of(me_z * NQ, NQ), NQ), :]
        else:
            wait_copy(zland.at[r], z_sems.at[r])
            block = zland[r]
        for j in range(chunks):
            wide16[r, pl.ds(j, NQ, stride=PITCH), :] = block[:, j * LANES : (j + 1) * LANES].astype(jnp.float32)
        fwd[r] = wide16[r].reshape(NQ, PITCH, LANES).astype(jnp.bfloat16)

        def send(a, q, device):
            remote(
                fwd.at[r, q, pl.ds(0, chunks)],
                recv1.at[r, me_p, pl.ds(0, chunks)],
                send_sem,
                plane1_sems.at[r],
                device,
            )

        each_in_plane(0, send)
        recv1[r, me_p] = fwd[r, me_q]

    with jax.named_scope("combine"):
        over_experts = jnp.exp(logits - jnp.max(logits, axis=0, keepdims=True))
        combine = over_experts / jnp.sum(over_experts, axis=0, keepdims=True)
        comb_ref[...] = combine.T.astype(jnp.bfloat16)

    half = w_in.shape[1]
    keep = (me_dp == 0).astype(jnp.float32)

    def gather(r):
        at = order.index(r) * NP
        wait_copy(recv1.at[r, pl.ds(0, NP - 1), pl.ds(0, chunks)], plane1_sems.at[r])
        wide32[...] = recv1[r].astype(jnp.float32).reshape(wide32.shape)
        for j in range(chunks):
            x_ref[at : at + NP, j * LANES : (j + 1) * LANES] = wide32[
                pl.ds(j, NP, stride=PITCH), :
            ].astype(jnp.bfloat16)

    def multiply(batch):
        start = order.index(BATCHES[batch][0]) * NP
        n = len(BATCHES[batch]) * NP
        rows = slice(start, start + n)
        if batch == 0:
            for load in loads[2:]:
                load.wait()
        for at in range(0, half, TILE1):
            bias = b_in[:, pl.ds(pl.multiple_of(me_dp * half + at, LANES), TILE1)].astype(jnp.float32)
            v = jnp.dot(x_ref[rows, :], w_in[:, at : at + TILE1], preferred_element_type=jnp.float32) + bias
            hid[rows, at : at + TILE1] = gelu(v).astype(jnp.bfloat16)
        for at in range(0, width, TILE2):
            y = jnp.dot(hid[rows, :], w_out[:, at : at + TILE2], preferred_element_type=jnp.float32)
            y = y + keep * b_out[:, at : at + TILE2].astype(jnp.float32)
            for c in range(TILE2 // LANES):
                wide_rows[pl.ds(start * PITCH + at // LANES + c, n, stride=PITCH), :] = y[
                    :, c * LANES : (c + 1) * LANES
                ]

    def scatter(r):
        first = order.index(r) * NP * PITCH
        send2[r] = wide_rows[first : first + NP * PITCH, :].reshape(NP, PITCH, LANES).astype(jnp.bfloat16)

        def send(a, q, device):
            remote(
                send2.at[r, a * NQ + q, pl.ds(0, chunks)],
                recv2.at[r, me_p, pl.ds(0, chunks)],
                send_sem,
                plane2_sems.at[r],
                device,
            )

        each_in_plane(r if r in DIRECT else 0, send)
        if r not in DIRECT:
            recv2[r, me_p] = send2[r, me_p]

    def reduce(r):
        rows = NP if r in DIRECT else NP - 1
        wait_copy(recv2.at[r, pl.ds(0, rows), pl.ds(0, chunks)], plane2_sems.at[r])
        pair = recv2[r, :NQ].astype(jnp.float32) + recv2[r, NQ:].astype(jnp.float32)
        wide16[r] = pair.reshape(NQ * PITCH, LANES)
        for j in range(chunks):
            total[r, :, j * LANES : (j + 1) * LANES] = wide16[r, pl.ds(j, NQ, stride=PITCH), :].astype(jnp.bfloat16)
        back = (NZ - r) % NZ
        if r == 0 or r in DIRECT:
            eo[expert_rows(back), :] = total[r]
        else:
            remote(total.at[r], eland.at[back], send_sem, eo_sem, along_z(r)[1])

    def expert_rows(d):
        return pl.ds(pl.multiple_of(lax.rem(me_z + d, NZ) * NQ, NQ), NQ)

    order = sum(BATCHES, ())
    actions = {"f": forward, "g": gather, "m": multiply, "s": scatter, "r": reduce}
    for step in STEPS:
        with jax.named_scope(step):
            actions[step[0]](int(step[1]))

    relayed = [r for r in COLUMN if r not in DIRECT]
    with jax.named_scope("eo"):
        wait_copy(zland.at[pl.ds(0, len(relayed))], eo_sem)
        for r in relayed:
            eo[expert_rows(NZ - r), :] = eland[NZ - r]
    with jax.named_scope("tail"):
        for sent in (recv1, recv2):
            wait_copy(sent.at[:, pl.ds(0, NP - 1), pl.ds(0, chunks)], send_sem)
        for r in DIRECT:
            wait_copy(recv1.at[r, 0, pl.ds(0, chunks)], send_sem)
        wait_copy(zland.at[pl.ds(0, NZ - 1)], send_sem)
        wait_copy(zland.at[pl.ds(0, len(relayed))], send_sem)


def mix_kernel(combine, expert_out, out_hbm, mixed, sems):
    count = sems.shape[0]
    tile = mixed.shape[1] // count
    writes = []
    for i in range(count):
        columns = pl.ds(i * tile, tile)
        mixed[:, columns] = jnp.dot(
            combine[...], expert_out[:, columns], preferred_element_type=jnp.float32
        ).astype(mixed.dtype)
        write = pltpu.make_async_copy(mixed.at[:, columns], out_hbm.at[0, :, columns], sems.at[i])
        write.start()
        writes.append(write)
    for write in writes:
        write.wait()


def shards(tokens, router, w_in, b_in, w_out, b_out):
    images, m, width = tokens.shape
    n_ex = NZ * NQ
    n = NZ * NP
    assert images == 1 and w_in.shape[0] == 1 and router.shape[1] == n_ex
    half = w_in.shape[2]
    bf16, f32 = jnp.bfloat16, jnp.float32
    dma = pltpu.SemaphoreType.DMA
    combine, expert_out = pl.pallas_call(
        kernel,
        out_shape=[
            pltpu.VMEM((m, n_ex), bf16),
            pltpu.VMEM((n_ex, width), bf16),
        ],
        in_specs=[pl.BlockSpec(memory_space=pltpu.HBM)] * 6,
        out_specs=[pl.BlockSpec(memory_space=pltpu.VMEM)] * 2,
        scratch_shapes=[
            pltpu.VMEM((m, width), bf16),
            pltpu.VMEM(router.shape, bf16),
            pltpu.VMEM(w_in.shape[1:], bf16),
            pltpu.VMEM(b_in.shape, bf16),
            pltpu.VMEM(w_out.shape[1:], bf16),
            pltpu.VMEM(b_out.shape, bf16),
            pltpu.VMEM((n_ex, m), f32),
            pltpu.VMEM((n_ex, width), bf16),
            pltpu.VMEM((NZ, NQ, width), bf16),
            pltpu.VMEM((NZ, NQ * PITCH, LANES), f32),
            pltpu.VMEM((NZ, NQ, PITCH, LANES), bf16),
            pltpu.VMEM((NZ, NP, PITCH, LANES), bf16),
            pltpu.VMEM((NP * PITCH, LANES), f32),
            pltpu.VMEM((n, width), bf16),
            pltpu.VMEM((n, half), bf16),
            pltpu.VMEM((n * PITCH, LANES), f32),
            pltpu.VMEM((NZ, NP, PITCH, LANES), bf16),
            pltpu.VMEM((NZ, NP, PITCH, LANES), bf16),
            pltpu.VMEM((NZ, NQ, width), bf16),
            pltpu.VMEM((NZ, NQ, width), bf16),
            dma((2,)),
            dma,
            dma((NZ,)),
            dma((NZ,)),
            dma((NZ,)),
            dma,
        ],
        compiler_params=pltpu.CompilerParams(
            collective_id=0, has_side_effects=True, vmem_limit_bytes=60 * 1024 * 1024
        ),
    )(tokens, router, w_in, b_in, w_out, b_out)
    tile = 2 * LANES
    return pl.pallas_call(
        mix_kernel,
        out_shape=jax.ShapeDtypeStruct(tokens.shape, bf16),
        in_specs=[pl.BlockSpec(memory_space=pltpu.VMEM)] * 2,
        out_specs=pl.BlockSpec(memory_space=pltpu.HBM),
        scratch_shapes=[
            pltpu.VMEM((m, width), bf16),
            dma((width // tile,)),
        ],
        compiler_params=pltpu.CompilerParams(vmem_limit_bytes=8 * 1024 * 1024),
    )(combine, expert_out)


def solution(mesh):
    return jax.shard_map(
        shards,
        mesh=mesh,
        in_specs=(
            P(("dp", "expert"), None, None),
            P(),
            P("expert", None, "dp"),
            P("expert", None),
            P("expert", "dp", None),
            P("expert", None),
        ),
        out_specs=P(("dp", "expert"), None, None),
        check_vma=False,
    )
```

```python
import functools

import jax
import jax.numpy as jnp
from jax import lax
from jax.experimental import pallas as pl
from jax.experimental.pallas import tpu as pltpu
from jax.sharding import PartitionSpec as P

MESH = pl.DeviceIdType.MESH
LANES = 128
PITCH = 16
NY, NZ, QUAD = 4, 8, 4
NQ = NY * QUAD
NP = 2 * NQ
COLUMN = (4, 1, 7, 2, 6, 3, 5)
BATCHES = ((0, 4, 1, 7), (3, 5, 2, 6))
DIRECT = ()
STEPS = ("f0", "f4", "f1", "f7", "f2", "f6", "f3", "f5", "g0", "g4", "g1", "g7", "m0", "s4", "s1", "s7", "g3", "g5", "g2", "g6", "m1", "s3", "s5", "r4", "r1", "r7", "s2", "s6", "s0", "r3", "r5", "r2", "r6", "r0")
FAR = True
MIX_TILES = 4
TILE1 = 256
TILE2 = 256


def gelu(v):
    return v * (1.0 + lax.erf(v * (0.5**0.5))) * 0.5


def wait_copy(ref, sem):
    pltpu.make_async_copy(ref, ref, sem).wait()


def kernel(
    tokens_hbm,
    router_hbm,
    w_in_hbm,
    b_in_hbm,
    w_out_hbm,
    b_out_hbm,
    comb_ref,
    eo,
    tok,
    router,
    w_in,
    b_in,
    w_out,
    b_out,
    permuted,
    send1,
    zland,
    wide16,
    fwd,
    recv1,
    wide32,
    x_ref,
    hid,
    wide_rows,
    send2,
    recv2,
    total,
    eland,
    load_sems,
    send_sem,
    z_sems,
    plane1_sems,
    plane2_sems,
    eo_sem,
):
    me_dp = lax.axis_index("dp")
    me_ex = lax.axis_index("expert")
    me_y = me_ex // (NZ * QUAD)
    me_z = lax.rem(me_ex // QUAD, NZ)
    me_quad = lax.rem(me_ex, QUAD)
    me_xh, me_core = me_quad // 2, lax.rem(me_quad, 2)
    me_q = me_y * QUAD + me_quad
    me_p = me_dp * NQ + me_q
    width = tok.shape[1]
    chunks = width // LANES

    def along_z(d):
        z = lax.rem(me_z + d, NZ)
        return z, (me_dp, me_y * (NZ * QUAD) + z * QUAD + me_quad)

    ys = [lax.rem(me_y + dy, NY) for dy in range(NY)]
    quads = [lax.rem(me_xh + dx, 2) * 2 + lax.rem(me_core + dc, 2) for dc in range(2) for dx in range(2)]
    dps = [me_dp, 1 - me_dp]
    plane = []
    def hops(t):
        dy, da, dx = t % NY, t // NY % 2, t // (2 * NY) % 2
        return min(dy, NY - dy) + (1 if da else 2 * dx)

    for t in sorted(range(NP - 1, -1, -1), key=hops, reverse=FAR):
        y, a, quad = ys[t % NY], dps[t // NY % 2], quads[t // (2 * NY)]
        plane.append((a, y * QUAD + quad, y * (NZ * QUAD) + quad))

    def each_in_plane(d, action):
        z = lax.rem(me_z + d, NZ) * QUAD
        for a, q, ex in plane[:-1]:
            action(a, q, (a, ex + z))

    def remote(src, dst, send_sem, recv_sem, device):
        pltpu.make_async_remote_copy(
            src_ref=src,
            dst_ref=dst,
            send_sem=send_sem,
            recv_sem=recv_sem,
            device_id=device,
            device_id_type=MESH,
        ).start()

    loads = [
        pltpu.make_async_copy(tokens_hbm.at[0], tok, load_sems.at[0]),
        pltpu.make_async_copy(router_hbm, router, load_sems.at[0]),
        pltpu.make_async_copy(w_in_hbm.at[0], w_in, load_sems.at[1]),
        pltpu.make_async_copy(b_in_hbm, b_in, load_sems.at[1]),
        pltpu.make_async_copy(w_out_hbm.at[0], w_out, load_sems.at[1]),
        pltpu.make_async_copy(b_out_hbm, b_out, load_sems.at[1]),
    ]
    loads[0].start()
    loads[1].start()
    barrier = pltpu.get_barrier_semaphore()

    def greet(device):
        pl.semaphore_signal(barrier, inc=1, device_id=device, device_id_type=MESH)

    with jax.named_scope("greet"):
        for d in COLUMN:
            greet(along_z(d)[1])
        each_in_plane(0, lambda a, q, device: greet(device))

    for load in loads[2:]:
        load.start()

    with jax.named_scope("waittok"):
        loads[0].wait()
        loads[1].wait()
    with jax.named_scope("dispatch"):
        logits = jnp.dot(tok[...], router[...], preferred_element_type=jnp.float32).T
        for y in range(NY):
            for z in range(NZ):
                at = (y * NZ + z) * QUAD
                permuted[z * NQ + y * QUAD : z * NQ + (y + 1) * QUAD, :] = logits[at : at + QUAD, :]
        logits = permuted[...]
        over_tokens = jnp.exp(logits - jnp.max(logits, axis=1, keepdims=True))
        dispatch = (over_tokens / jnp.sum(over_tokens, axis=1, keepdims=True)).astype(jnp.bfloat16)
        send1[...] = jnp.dot(dispatch, tok[...], preferred_element_type=jnp.float32).astype(jnp.bfloat16)

    with jax.named_scope("barwait"):
        pl.semaphore_wait(barrier, NZ - 1 + NP - 1)

    with jax.named_scope("sendz"):
        for d in COLUMN:
            z, device = along_z(d)
            back = NZ - d
            remote(
                send1.at[pl.ds(pl.multiple_of(z * NQ, NQ), NQ)],
                zland.at[back],
                send_sem,
                z_sems.at[back],
                device,
            )

    def forward(r):
        if r == 0:
            block = send1[pl.ds(pl.multiple_of(me_z * NQ, NQ), NQ), :]
        else:
            wait_copy(zland.at[r], z_sems.at[r])
            block = zland[r]
        for j in range(chunks):
            wide16[r, pl.ds(j, NQ, stride=PITCH), :] = block[:, j * LANES : (j + 1) * LANES].astype(jnp.float32)
        fwd[r] = wide16[r].reshape(NQ, PITCH, LANES).astype(jnp.bfloat16)

        def send(a, q, device):
            remote(
                fwd.at[r, q, pl.ds(0, chunks)],
                recv1.at[r, me_p, pl.ds(0, chunks)],
                send_sem,
                plane1_sems.at[r],
                device,
            )

        each_in_plane(0, send)
        recv1[r, me_p] = fwd[r, me_q]

    with jax.named_scope("combine"):
        over_experts = jnp.exp(logits - jnp.max(logits, axis=0, keepdims=True))
        combine = over_experts / jnp.sum(over_experts, axis=0, keepdims=True)
        comb_ref[...] = combine.T.astype(jnp.bfloat16)

    half = w_in.shape[1]
    keep = (me_dp == 0).astype(jnp.float32)

    def gather(r):
        at = order.index(r) * NP
        wait_copy(recv1.at[r, pl.ds(0, NP - 1), pl.ds(0, chunks)], plane1_sems.at[r])
        wide32[...] = recv1[r].astype(jnp.float32).reshape(wide32.shape)
        for j in range(chunks):
            x_ref[at : at + NP, j * LANES : (j + 1) * LANES] = wide32[
                pl.ds(j, NP, stride=PITCH), :
            ].astype(jnp.bfloat16)

    def multiply(batch):
        start = order.index(BATCHES[batch][0]) * NP
        n = len(BATCHES[batch]) * NP
        rows = slice(start, start + n)
        if batch == 0:
            for load in loads[2:]:
                load.wait()
        for at in range(0, half, TILE1):
            bias = b_in[:, pl.ds(pl.multiple_of(me_dp * half + at, LANES), TILE1)].astype(jnp.float32)
            v = jnp.dot(x_ref[rows, :], w_in[:, at : at + TILE1], preferred_element_type=jnp.float32) + bias
            hid[rows, at : at + TILE1] = gelu(v).astype(jnp.bfloat16)
        for at in range(0, width, TILE2):
            y = jnp.dot(hid[rows, :], w_out[:, at : at + TILE2], preferred_element_type=jnp.float32)
            y = y + keep * b_out[:, at : at + TILE2].astype(jnp.float32)
            for c in range(TILE2 // LANES):
                wide_rows[pl.ds(start * PITCH + at // LANES + c, n, stride=PITCH), :] = y[
                    :, c * LANES : (c + 1) * LANES
                ]

    def scatter(r):
        first = order.index(r) * NP * PITCH
        send2[r] = wide_rows[first : first + NP * PITCH, :].reshape(NP, PITCH, LANES).astype(jnp.bfloat16)

        def send(a, q, device):
            remote(
                send2.at[r, a * NQ + q, pl.ds(0, chunks)],
                recv2.at[r, me_p, pl.ds(0, chunks)],
                send_sem,
                plane2_sems.at[r],
                device,
            )

        each_in_plane(r if r in DIRECT else 0, send)
        if r not in DIRECT:
            recv2[r, me_p] = send2[r, me_p]

    def reduce(r):
        rows = NP if r in DIRECT else NP - 1
        wait_copy(recv2.at[r, pl.ds(0, rows), pl.ds(0, chunks)], plane2_sems.at[r])
        pair = recv2[r, :NQ].astype(jnp.float32) + recv2[r, NQ:].astype(jnp.float32)
        wide16[r] = pair.reshape(NQ * PITCH, LANES)
        for j in range(chunks):
            total[r, :, j * LANES : (j + 1) * LANES] = wide16[r, pl.ds(j, NQ, stride=PITCH), :].astype(jnp.bfloat16)
        back = (NZ - r) % NZ
        if r == 0 or r in DIRECT:
            eo[expert_rows(back), :] = total[r]
        else:
            remote(total.at[r], eland.at[back], send_sem, eo_sem, along_z(r)[1])

    def expert_rows(d):
        return pl.ds(pl.multiple_of(lax.rem(me_z + d, NZ) * NQ, NQ), NQ)

    order = sum(BATCHES, ())
    actions = {"f": forward, "g": gather, "m": multiply, "s": scatter, "r": reduce}
    for step in STEPS:
        with jax.named_scope(step):
            actions[step[0]](int(step[1]))

    relayed = [r for r in COLUMN if r not in DIRECT]
    with jax.named_scope("eo"):
        wait_copy(zland.at[pl.ds(0, len(relayed))], eo_sem)
        for r in relayed:
            eo[expert_rows(NZ - r), :] = eland[NZ - r]
    with jax.named_scope("tail"):
        for sent in (recv1, recv2):
            wait_copy(sent.at[:, pl.ds(0, NP - 1), pl.ds(0, chunks)], send_sem)
        for r in DIRECT:
            wait_copy(recv1.at[r, 0, pl.ds(0, chunks)], send_sem)
        wait_copy(zland.at[pl.ds(0, NZ - 1)], send_sem)
        wait_copy(zland.at[pl.ds(0, len(relayed))], send_sem)


def mix_kernel(combine, expert_out, out_hbm, mixed, sems):
    count = sems.shape[0]
    tile = mixed.shape[0] // count
    writes = []
    for i in range(count):
        rows = pl.ds(i * tile, tile)
        mixed[rows, :] = jnp.dot(
            combine[rows, :], expert_out[...], preferred_element_type=jnp.float32
        ).astype(mixed.dtype)
        write = pltpu.make_async_copy(mixed.at[rows], out_hbm.at[0, rows], sems.at[i])
        write.start()
        writes.append(write)
    for write in writes:
        write.wait()


def shards(tokens, router, w_in, b_in, w_out, b_out):
    images, m, width = tokens.shape
    n_ex = NZ * NQ
    n = NZ * NP
    assert images == 1 and w_in.shape[0] == 1 and router.shape[1] == n_ex
    half = w_in.shape[2]
    bf16, f32 = jnp.bfloat16, jnp.float32
    dma = pltpu.SemaphoreType.DMA
    combine, expert_out = pl.pallas_call(
        kernel,
        out_shape=[
            pltpu.VMEM((m, n_ex), bf16),
            pltpu.VMEM((n_ex, width), bf16),
        ],
        in_specs=[pl.BlockSpec(memory_space=pltpu.HBM)] * 6,
        out_specs=[pl.BlockSpec(memory_space=pltpu.VMEM)] * 2,
        scratch_shapes=[
            pltpu.VMEM((m, width), bf16),
            pltpu.VMEM(router.shape, bf16),
            pltpu.VMEM(w_in.shape[1:], bf16),
            pltpu.VMEM(b_in.shape, bf16),
            pltpu.VMEM(w_out.shape[1:], bf16),
            pltpu.VMEM(b_out.shape, bf16),
            pltpu.VMEM((n_ex, m), f32),
            pltpu.VMEM((n_ex, width), bf16),
            pltpu.VMEM((NZ, NQ, width), bf16),
            pltpu.VMEM((NZ, NQ * PITCH, LANES), f32),
            pltpu.VMEM((NZ, NQ, PITCH, LANES), bf16),
            pltpu.VMEM((NZ, NP, PITCH, LANES), bf16),
            pltpu.VMEM((NP * PITCH, LANES), f32),
            pltpu.VMEM((n, width), bf16),
            pltpu.VMEM((n, half), bf16),
            pltpu.VMEM((n * PITCH, LANES), f32),
            pltpu.VMEM((NZ, NP, PITCH, LANES), bf16),
            pltpu.VMEM((NZ, NP, PITCH, LANES), bf16),
            pltpu.VMEM((NZ, NQ, width), bf16),
            pltpu.VMEM((NZ, NQ, width), bf16),
            dma((2,)),
            dma,
            dma((NZ,)),
            dma((NZ,)),
            dma((NZ,)),
            dma,
        ],
        compiler_params=pltpu.CompilerParams(
            collective_id=0, has_side_effects=True, vmem_limit_bytes=60 * 1024 * 1024
        ),
    )(tokens, router, w_in, b_in, w_out, b_out)
    return pl.pallas_call(
        mix_kernel,
        out_shape=jax.ShapeDtypeStruct(tokens.shape, bf16),
        in_specs=[pl.BlockSpec(memory_space=pltpu.VMEM)] * 2,
        out_specs=pl.BlockSpec(memory_space=pltpu.HBM),
        scratch_shapes=[
            pltpu.VMEM((m, width), bf16),
            dma((MIX_TILES,)),
        ],
        compiler_params=pltpu.CompilerParams(vmem_limit_bytes=8 * 1024 * 1024),
    )(combine, expert_out)


def solution(mesh):
    return jax.shard_map(
        shards,
        mesh=mesh,
        in_specs=(
            P(("dp", "expert"), None, None),
            P(),
            P("expert", None, "dp"),
            P("expert", None),
            P("expert", "dp", None),
            P("expert", None),
        ),
        out_specs=P(("dp", "expert"), None, None),
        check_vma=False,
    )
```
